256 devices in a mesh: expert: 64 (over z, y, core), dp: 4 (over x).
Axes of the slice: x: 4, y: 4, z: 8, core: 2. Of those that a mesh axis runs over, the one named last changes fastest.
Arguments:
- tokens: bfloat16 [16384, 2880], P(('expert', 'dp')), may hold values from -6 to 6
- expert_ids: int32 [16384, 4], P(('expert', 'dp')), may hold values from 0 to 63, all different within a row; in each aligned block of 64 rows (0 to 63, 64 to 127, ...) at most 6 rows name the same one
- gate_logits: float32 [16384, 4], P(('expert', 'dp')), may hold values from -3 to 3
- w_gate: bfloat16 [64, 2880, 1536], P('expert', None, 'dp'), may hold values from -0.109375 to 0.109375
- w_up: bfloat16 [64, 2880, 1536], P('expert', None, 'dp'), may hold values from -0.109375 to 0.109375
- w_down: bfloat16 [64, 1536, 2880], P('expert', 'dp'), may hold values from -0.15625 to 0.15625
Outputs:
- mixed: bfloat16 [16384, 2880], P(('expert', 'dp'))
The draws below stay inside these ranges and needn't reach their ends.
Inputs may be any that keep to these rules, and one draw needn't show every extreme that they name: `expert_ids`: each row names 4 different experts. Among the 64 rows of one device no expert is named more than 6 times, and every expert is named somewhere.
All inputs are finite; a program needn't handle non-finite values.
Results may differ from the reference program's by a relative error of at most 0.012.
Values may be sent and summed in bfloat16 or wider, within the bound.
No kernel may reach another device: no remote copies, remote signals or barrier semaphores. Data moves between devices by JAX's collectives and lax.ppermute only.
A program may use at most 128 MiB of HBM per device.

```python
import math
import jax
import jax.numpy as jnp
import numpy as np
from jax import lax

D = 2880
FF = 1536
TOP = 4
TOK_DEV = 64
EXPERTS = 64
CAP = 6
TOKENS = 16384
N_EXPERT = 64
N_DP = 4


def levels(rng, dims, split, smallest, largest):
    loudness, own = 1.0, jax.random.fold_in(rng, 6)
    for dim, shards_of in split:
        steps = jnp.exp(jax.random.uniform(jax.random.fold_in(own, dim), (shards_of,), jnp.float32, smallest / len(split), largest / len(split)))
        loudness = loudness * jnp.repeat(steps, dims[dim] // shards_of).reshape([-1 if axis == dim else 1 for axis in range(len(dims))])
    return loudness


def shared_out(key, own, number, rows, count, top, most, lean):
    order = jax.random.permutation(key, count)
    crowded, common = shares(count, rows * top, most, lean, True), shares(count, rows * top, most, lean, False)
    places = jnp.arange(count)

    def named(tallies, rotation):
        used = int((tallies > 0).sum())
        fixed = max(1, used // 4)
        moved = fixed + (places - fixed + rotation * (used - fixed)) % max(1, count - fixed)
        return jnp.zeros((count,), jnp.int32).at[order[jnp.where(places < fixed, places, moved)]].set(jnp.asarray(tallies, jnp.int32))

    tallies = jnp.where(number % 4 == 0, named(crowded, number // 4), named(common, number - number // 4 - 1))
    mixed = jax.random.permutation(jax.random.fold_in(own, 3), count)
    source_of, taker = mixed[0:count // 2 * 2:2], mixed[1:count // 2 * 2:2]
    room = jnp.minimum(tallies[source_of] - 1, most - tallies[taker]) // 2
    room = jnp.where((source_of == order[0]) | (taker == order[0]) | (tallies[taker] == 0), 0, jnp.maximum(room, 0))
    moved = jax.random.randint(jax.random.fold_in(own, 4), (count // 2,), 0, 1 << 20) % (room + 1)
    tallies = tallies.at[source_of].add(-moved).at[taker].add(moved)
    labels = jnp.searchsorted(jnp.cumsum(tallies), jnp.arange(rows * top), side="right").astype(jnp.int32)
    table = labels.reshape(top, rows).T
    table = table[jax.random.permutation(jax.random.fold_in(own, 1), rows)]
    rotation = jax.random.randint(jax.random.fold_in(own, 2), (rows, 1), 0, top)
    return jnp.take_along_axis(table, (jnp.arange(top)[None, :] + rotation) % top, axis=1)


def shares(amount, total, limit, skew, full):
    weights = [(1 << 20) // math.isqrt(standing ** skew) + 1 for standing in range(1, amount + 1)]
    largest = limit if full else min(limit, max(-(-total // amount), total * weights[0] // sum(weights)))
    least = 1 if total - largest >= amount - 1 else 0
    given, spare = [largest] + [least] * (amount - 1), total - largest - least * (amount - 1)
    while spare > 0:
        movable = [i for i in range(1, amount) if given[i] < largest] or [i for i in range(1, amount) if given[i] < limit]
        mass, left = sum([weights[i] for i in movable]), spare
        for i in movable:
            addition = min(limit - given[i], max(1, left * weights[i] // mass), spare)
            given[i] = given[i] + addition
            spare = spare - addition
    return np.array(given)


def normal_values(key, extent, scale, most, split=(), kind=jnp.bfloat16):
    result = jax.random.normal(key, extent, jnp.float32) * scale
    if len(split) > 0:
        result = levels(key, extent, split, -0.22, 0.18) * result
    return jnp.clip(result, min=-most, max=most).astype(kind)


def setup_inputs(seed: int = 0) -> dict:
    key_list = jax.random.split(jax.random.key(seed), 7)
    tokens = normal_values(key_list[0], (TOKENS, D), 1.0, 6.0, ((0, 256),))
    expert_ids_keys = jax.random.split(jax.random.fold_in(key_list[1], 1), TOKENS // TOK_DEV)
    expert_ids_turns = jax.random.permutation(jax.random.fold_in(key_list[1], 3), TOKENS // TOK_DEV)
    expert_ids = jax.vmap(lambda own, number: shared_out(jax.random.fold_in(key_list[1], 2), own, number, TOK_DEV, EXPERTS, TOP, CAP, 2))(expert_ids_keys, expert_ids_turns).reshape((TOKENS, TOP))
    gate_logits = jnp.clip(jax.random.uniform(key_list[2], (TOKENS, TOP), jnp.float32, -3.0, 3.0) * levels(key_list[2], (TOKENS, TOP), ((0, 256),), -0.4, 0.0), -3.0, 3.0)
    w_gate = normal_values(key_list[3], (EXPERTS, D, FF), D ** -0.5, 0.109375, ((0, 64), (2, 4)))
    w_up = normal_values(key_list[4], (EXPERTS, D, FF), D ** -0.5, 0.109375, ((0, 64), (2, 4)))
    w_down = normal_values(key_list[5], (EXPERTS, FF, D), FF ** -0.5, 0.15625, ((0, 64), (1, 4)))
    return dict(tokens=tokens, expert_ids=expert_ids, gate_logits=gate_logits, w_gate=w_gate, w_up=w_up, w_down=w_down)


def expert_rows(rows_in, gate_w, up_w, down_w):
    quarter = gate_w.shape[1] // N_DP
    summed = jnp.zeros((rows_in.shape[0], down_w.shape[1]), jnp.float32)
    for index_q in range(N_DP):
        low_col = index_q * quarter
        high_col = low_col + quarter
        gate_val = jnp.dot(rows_in, gate_w[:, low_col:high_col], preferred_element_type=jnp.float32)
        up_val = jnp.dot(rows_in, up_w[:, low_col:high_col], preferred_element_type=jnp.float32)
        hidden = ((up_val + 1.0) * gate_val * jax.nn.sigmoid(1.702 * gate_val)).astype(jnp.bfloat16)
        partial_value = jnp.dot(hidden, down_w[low_col:high_col], preferred_element_type=jnp.float32).astype(jnp.bfloat16)
        summed = summed + lax.optimization_barrier(partial_value).astype(jnp.float32)
    return summed.astype(jnp.bfloat16)


def reference(tokens, expert_ids, gate_logits, w_gate, w_up, w_down):
    n_assign = TOKENS * TOP
    flat_ids = expert_ids.reshape(-1).astype(jnp.int32)
    sorter = jnp.argsort(flat_ids, stable=True).astype(jnp.int32)
    counts = jnp.sum((flat_ids[:, None] == jnp.arange(EXPERTS, dtype=jnp.int32)[None, :]).astype(jnp.int32), axis=0)
    starts = (jnp.cumsum(counts) - counts).astype(jnp.int32)
    longest = N_EXPERT * N_DP * CAP
    padded_order = jnp.concatenate([sorter, jnp.zeros((longest,), jnp.int32)])

    def per_expert(expert):
        chosen = lax.dynamic_slice_in_dim(padded_order, starts[expert], longest)
        rows_in = tokens[chosen // TOP]
        return expert_rows(rows_in, w_gate[expert], w_up[expert], w_down[expert])

    outputs_all = lax.map(per_expert, jnp.arange(EXPERTS, dtype=jnp.int32))
    inverse = jnp.zeros((n_assign,), jnp.int32).at[sorter].set(jnp.arange(n_assign, dtype=jnp.int32))
    rank_in = (inverse - starts[flat_ids]).astype(jnp.int32)
    picked = outputs_all.reshape(-1, D)[flat_ids * longest + rank_in]
    gate_wts = jnp.exp(gate_logits.astype(jnp.float32))
    gate_wts = gate_wts / jnp.sum(gate_wts, axis=1, keepdims=True)
    mixed = jnp.sum(picked.reshape(TOKENS, TOP, D).astype(jnp.float32) * gate_wts[:, :, None], axis=1)
    return mixed.astype(jnp.bfloat16)
```

```python
import jax
import jax.numpy as jnp
from jax import lax
from jax.experimental import pallas as pl
from jax.sharding import PartitionSpec as P

CHUNKS = (2, 2, 2)
SPLIT = "hPP"
CUT = (0, 2880)
PAIRS = {"P": ((0, 1), (1, 0), (2, 3), (3, 2)), "A": ((0, 3), (3, 0), (1, 2), (2, 1))}
F32, BF16 = jnp.float32, jnp.bfloat16


def rows_of(ref):
    return [ref[...]] if len(ref.shape) == 2 else [ref[i] for i in range(ref.shape[0])]


def hidden_body(*refs):
    ins, (gate_w, up_w, send, keep) = refs[:-4], refs[-4:]
    rows = jnp.concatenate([piece for ref in ins for piece in rows_of(ref)], axis=0)
    gate = jnp.dot(rows, gate_w[...], preferred_element_type=F32)
    up = jnp.dot(rows, up_w[...], preferred_element_type=F32)
    hidden = ((up + 1.0) * gate * jax.nn.sigmoid(1.702 * gate)).astype(BF16)
    half = send.shape[0]
    send[...] = hidden[:half]
    keep[...] = hidden[half:]


def hidden_rows(ins, gate_w, up_w):
    _, half, width = ins[0].shape
    units = gate_w.shape[1]
    return pl.pallas_call(
        hidden_body,
        out_shape=[jax.ShapeDtypeStruct((4 * half, units), BF16)] * 2,
        name="hidden",
        cost_estimate=pl.CostEstimate(flops=32 * half * width * units, transcendentals=8 * half * units, bytes_accessed=8 << 20),
    )(*ins, gate_w, up_w)


def down_body(keep, recv, own_w, *refs):
    pieces, (own, adjacent) = refs[:-2], refs[-2:]
    nt = (((1,), (1,)), ((), ()))
    half = own.shape[1]
    at = 0
    for piece in pieces:
        end = at + piece.shape[0]
        total = lax.dot_general(keep[...], own_w[at:end], nt, preferred_element_type=F32)
        total += lax.dot_general(recv[...], piece[...], nt, preferred_element_type=F32)
        total = total.astype(BF16)
        for index, ref in enumerate((own, adjacent)):
            for side in range(2):
                row = (2 * index + side) * half
                ref[side, :, at:end] = total[row:row + half]
        at = end


def down_rows(keep, recv, own_w, pieces):
    rows = keep.shape[0]
    width, units = own_w.shape
    pair = jax.ShapeDtypeStruct((2, rows // 4, width), BF16)
    return pl.pallas_call(
        down_body,
        out_shape=[pair, pair],
        name="down",
        cost_estimate=pl.CostEstimate(flops=4 * rows * width * units, transcendentals=0, bytes_accessed=6 << 20),
    )(keep, recv, own_w, *pieces)


def layer(tokens, expert_ids, gate_logits, w_gate, w_up, w_down):
    n_rows, width = tokens.shape
    n_exp = lax.axis_size("expert")

    def send(value, way):
        return lax.ppermute(value, "dp", PAIRS[way])

    def exchange(value):
        return lax.all_to_all(value, "expert", split_axis=0, concat_axis=0, tiled=True)

    named = expert_ids[None, :, :] == jnp.arange(n_exp, dtype=jnp.int32)[:, None, None]
    member = jnp.any(named, axis=2)
    tri = (jnp.arange(n_rows)[:, None] < jnp.arange(n_rows)[None, :]).astype(BF16)
    rank = jnp.dot(member.astype(BF16), tri, preferred_element_type=F32)
    weights = jnp.exp(gate_logits)
    weights = weights / jnp.sum(weights, axis=1, keepdims=True)
    by_expert = jnp.sum(jnp.where(named, weights[None], 0.0), axis=2)
    gate_w, up_w, own_w = w_gate[0], w_up[0], w_down[0].T
    pieces = []
    for lo, hi in zip(CUT, CUT[1:]):
        cut = own_w[lo:hi]
        pieces.append(send(cut, "P"))

    base = 0
    rows_out = []
    for c, size in enumerate(CHUNKS):
        slots = base + jnp.arange(size, dtype=jnp.int32).astype(F32)
        onehot = (member[:, None, :] & (rank[:, None, :] == slots[None, :, None]))
        onehot = onehot.reshape(n_exp * size, n_rows)
        sent = jnp.dot(onehot.astype(BF16), tokens, preferred_element_type=F32).astype(BF16)
        sent = sent.reshape(n_exp, size, width)
        mid = exchange(sent)
        own = mid.reshape(2, n_exp * size // 2, width)
        partner = send(own, "P")
        adjacent = send(own, "A")
        if SPLIT[c] == "h":
            far = [send(partner[0], "A"), send(adjacent[1], "P")]
        elif SPLIT[c] == "A":
            far = [send(partner, "A")]
        else:
            far = [send(adjacent, "P")]
        away, keep = hidden_rows([partner, *far, own, adjacent], gate_w, up_w)
        recv = send(away, "P")
        mine, theirs = down_rows(keep, recv, own_w, pieces)
        other = send(theirs, "A")
        summed = (mine.astype(F32) + other.astype(F32)).astype(BF16).reshape(n_exp, size, width)
        back = exchange(summed).reshape(n_exp * size, width)
        scale = jnp.where(onehot.reshape(n_exp, size, n_rows), by_expert[:, None, :], 0.0).reshape(n_exp * size, n_rows)
        high = scale.astype(BF16)
        low = (scale - high.astype(F32)).astype(BF16)
        dims = (((0,), (0,)), ((), ()))
        rows_out.append(
            lax.dot_general(high, back, dims, preferred_element_type=F32)
            + lax.dot_general(low, back, dims, preferred_element_type=F32)
        )
        base += size
    return sum(rows_out).astype(BF16)


def solution(mesh):
    return jax.shard_map(
        layer,
        mesh=mesh,
        in_specs=(
            P(("expert", "dp"), None),
            P(("expert", "dp"), None),
            P(("expert", "dp"), None),
            P("expert", None, "dp"),
            P("expert", None, "dp"),
            P("expert", "dp", None),
        ),
        out_specs=P(("expert", "dp"), None),
        check_vma=False,
    )
```
